32 devices in a mesh: section: 4 (over y, x), cp: 4 (over z), tp: 2 (over core).
Axes of the slice: x: 2, y: 2, z: 4, core: 2. Of those that a mesh axis runs over, the one named last changes fastest.
Arguments:
- acts: bfloat16 [4, 512, 8192], P('section', 'cp', 'tp'), may hold values from -16 to 16
- keys: bfloat16 [4, 512, 1024], P('section', 'cp', 'tp'), may hold values from -4 to 4
- values: bfloat16 [4, 512, 1024], P('section', 'cp', 'tp'), may hold values from -6 to 6
- grads: bfloat16 [4, 512, 8192], P('section', 'cp', 'tp'), may hold values from -6 to 6
- docs: int32 [4, 512], P('section'), may hold values from 0 to 7, never falling along the last dimension, each value on 1 to 256 neighbouring positions
- order: int32 [4, 512], P('section'), may hold values from 0 to 511, each once within a row
Outputs:
- outputs: bfloat16 [4, 512, 8192], P('section', 'cp', 'tp')
- grad_query: bfloat16 [4, 512, 8192], P('section', 'cp', 'tp')
- grad_keys: bfloat16 [4, 512, 1024], P('section', 'cp', 'tp')
- grad_values: bfloat16 [4, 512, 1024], P('section', 'cp', 'tp')
The draws below stay inside these ranges and needn't reach their ends.
Inputs may be any that keep to these rules, and one draw needn't show every extreme that they name: `docs`: along positions of one section the document numbers never fall; each document holds 1 to 256 tokens. `order`: each section's row holds every position once.
All inputs are finite; a program needn't handle non-finite values.
Results may differ from the reference program's by a relative error of at most 0.0061.
Values may be sent and summed in bfloat16 or wider, within the bound.
A program may use at most 64 MiB of HBM per device.

```python
import math
import jax
import jax.numpy as jnp
import numpy as np
from jax import lax

HEADS = 64
KV_HEADS = 8
HEAD = 128
DOCS = 8
TOKENS = 512
SECTIONS = 4
DOC_MOST = 256
QW = 8192
KVW = 1024


def draw_acts(key, part):
    shape = (SECTIONS, TOKENS, HEADS * HEAD)
    result = jax.random.truncated_normal(jax.random.fold_in(key, 11), -4.0, 4.0, shape, jnp.float32)
    return result.astype(jnp.bfloat16)


def draw_keys(key, part):
    shape = (SECTIONS, TOKENS, KV_HEADS * HEAD)
    result = jax.random.truncated_normal(jax.random.fold_in(key, 13), -4.0, 4.0, shape, jnp.float32)
    return result.astype(jnp.bfloat16)


def block_levels(key, shape, split, least, largest):
    level = 1.0
    for dim, shards_of in split:
        steps = jax.random.uniform(jax.random.fold_in(jax.random.fold_in(key, 6), dim), (shards_of,), jnp.float32, least / len(split), largest / len(split))
        level = level * jnp.repeat(jnp.exp(steps), shape[dim] // shards_of).reshape((-1,) + (1,) * (len(shape) - 1 - dim))
    return level


def split_up(amount, total, reach, skew):
    weights = [(1 << 20) // math.isqrt(grade ** skew) + 1 for grade in range(2, amount + 1)]
    rest, counts = total - reach - (amount - 1), [1] * (amount - 1)
    while rest > 0:
        movable = [i for i in range(amount - 1) if counts[i] < reach]
        mass, left = sum([weights[i] for i in movable]), rest
        for i in movable:
            more = min(reach - counts[i], max(1, left * weights[i] // mass), rest)
            counts[i] = counts[i] + more
            rest = rest - more
    return np.array([reach] + counts)


def ragged(stream_key, count, total, limit, skew):
    if count == 2:
        one = jax.random.randint(stream_key, (), max(1, total - limit), min(limit, total - 1) + 1)
        return jnp.stack([one, total - one])
    sizes = jnp.asarray(split_up(count, total, limit, skew), jnp.int32)
    couples = (count - 1) // 2
    source_of, receiver = sizes[1:1 + 2 * couples:2], sizes[2:2 + 2 * couples:2]
    slack = jnp.minimum(source_of - 1, limit - receiver)
    shifted = jax.random.randint(jax.random.fold_in(stream_key, 1), (couples,), 0, 1 << 20) % (slack + 1)
    sizes = sizes.at[1:1 + 2 * couples:2].set(source_of - shifted).at[2:2 + 2 * couples:2].set(receiver + shifted)
    return sizes[jax.random.permutation(jax.random.fold_in(stream_key, 2), count)]


def bell_draw(own_key, shape, width, limit, shards=(), held_as=jnp.bfloat16):
    loudness = block_levels(own_key, shape, shards, -0.22, 0.18) if shards else 1.0
    entries = jax.random.normal(own_key, shape, jnp.float32) * width * loudness
    return jnp.minimum(jnp.maximum(entries, -limit), limit).astype(held_as)


def setup_inputs(seed: int = 0) -> dict:
    seeds = jax.random.split(jax.random.key(seed), 7)
    acts = draw_acts(jax.random.fold_in(seeds[6], 71), 0)
    keys = draw_keys(jax.random.fold_in(seeds[6], 71), 0)
    values = bell_draw(seeds[2], (SECTIONS, TOKENS, KVW), 1.0, 6.0, ((0, 4), (1, 4), (2, 2)))
    grads = bell_draw(seeds[3], (SECTIONS, TOKENS, QW), 1.0, 6.0, ((0, 4), (1, 4), (2, 2)))
    docs = jax.vmap(lambda own: jnp.searchsorted(jnp.cumsum(ragged(own, DOCS, TOKENS, DOC_MOST, 1)), jnp.arange(TOKENS), side="right"))(jax.random.split(seeds[4], SECTIONS)).reshape((SECTIONS, TOKENS)).astype(jnp.int32)
    order = jax.vmap(lambda own: jax.random.permutation(own, TOKENS))(jax.random.split(seeds[5], SECTIONS)).reshape((SECTIONS, TOKENS)).astype(jnp.int32)
    return {"acts": acts, "keys": keys, "values": values, "grads": grads, "docs": docs, "order": order}


def split_heads(block, kv_count):
    tokens = block.shape[0]
    group = block.shape[1] // (kv_count * HEAD)
    return block.reshape(tokens, kv_count, group, HEAD).transpose(1, 2, 0, 3).reshape(kv_count, group * tokens, HEAD)


def join_heads(rows, tokens):
    kv_count = rows.shape[0]
    group = rows.shape[1] // tokens
    return rows.reshape(kv_count, group, tokens, HEAD).transpose(2, 0, 1, 3).reshape(tokens, kv_count * group * HEAD)


def forward_part(flat_q, key, value, allowed):
    scale = HEAD ** -0.5
    rows_q = allowed.shape[0]
    scores = lax.dot_general(flat_q, key, (((1,), (1,)), ((), ())), preferred_element_type=jnp.float32) * scale
    scores = scores.reshape(-1, rows_q, key.shape[0])
    scores = jnp.where(allowed[None], scores, -jnp.inf)
    peak = jnp.max(scores, axis=2, keepdims=True)
    expd = jnp.exp(scores - peak)
    probs = (expd / jnp.sum(expd, axis=2, keepdims=True)).astype(jnp.bfloat16)
    probs = probs.reshape(flat_q.shape[0], key.shape[0])
    attended = jnp.dot(probs, value, preferred_element_type=jnp.float32)
    return probs, attended


def backward_part(probs, attended, flat_g, key, value):
    scale = HEAD ** -0.5
    delta = jnp.sum(flat_g.astype(jnp.float32) * attended, axis=1, keepdims=True)
    dprob = lax.dot_general(flat_g, value, (((1,), (1,)), ((), ())), preferred_element_type=jnp.float32)
    dscore = (probs.astype(jnp.float32) * (dprob - delta)).astype(jnp.bfloat16)
    dquery = jnp.dot(dscore, key, preferred_element_type=jnp.float32) * scale
    return dscore, dquery


def key_terms(probs, dscore, flat_q, flat_g):
    scale = HEAD ** -0.5
    dkey = lax.dot_general(dscore, flat_q, (((0,), (0,)), ((), ())), preferred_element_type=jnp.float32) * scale
    dvalue = lax.dot_general(probs, flat_g, (((0,), (0,)), ((), ())), preferred_element_type=jnp.float32)
    return dkey, dvalue


def section_pass(items):
    query, key, value, cotan, doc_row, order_row = items
    tokens = query.shape[0]
    kv_count = key.shape[1] // HEAD
    doc_all = jnp.take(doc_row, order_row)
    allowed = (doc_all[:, None] == doc_all[None, :]) & (order_row[None, :] <= order_row[:, None])
    q_rows = split_heads(query, kv_count)
    g_rows = split_heads(cotan, kv_count)
    k_heads = key.reshape(tokens, kv_count, HEAD).transpose(1, 0, 2)
    v_heads = value.reshape(tokens, kv_count, HEAD).transpose(1, 0, 2)

    def one_head(parts):
        probs, attended = forward_part(parts[0], parts[1], parts[2], allowed)
        dscore, dquery = backward_part(probs, attended, parts[3], parts[1], parts[2])
        dkey, dvalue = key_terms(probs, dscore, parts[0], parts[3])
        return attended, dquery, dkey, dvalue

    attended, dqueries, dkeys, dvalues = lax.map(one_head, (q_rows, k_heads, v_heads, g_rows))
    outputs = (query.astype(jnp.float32) + join_heads(attended, tokens)).astype(jnp.bfloat16)
    grad_query = (cotan.astype(jnp.float32) + join_heads(dqueries, tokens)).astype(jnp.bfloat16)
    grad_keys = dkeys.transpose(1, 0, 2).reshape(tokens, kv_count * HEAD).astype(jnp.bfloat16)
    grad_values = dvalues.transpose(1, 0, 2).reshape(tokens, kv_count * HEAD).astype(jnp.bfloat16)
    return outputs, grad_query, grad_keys, grad_values


def reference(acts, keys, values, grads, docs, order):
    arriving = jnp.roll(acts, 1, axis=0)
    returning = jnp.roll(grads, -1, axis=0)
    outputs, grad_query, grad_keys, grad_values = lax.map(section_pass, (arriving, keys, values, returning, docs, order))
    return (outputs, grad_query, grad_keys, grad_values)
```

```python
import functools

import jax
import jax.numpy as jnp
from jax import lax
from jax.experimental import pallas as pl
from jax.experimental.pallas import tpu as pltpu
from jax.sharding import PartitionSpec as P

HEAD = 128
DOCS = 8


def passed_along(block, axis, distance):
    devices = range(lax.axis_size(axis))
    route = [((i - distance) % len(devices), i) for i in devices]
    return lax.ppermute(block, axis, route)


def times(a, b, dims):
    return lax.dot_general(a, b, (dims, ((), ())), preferred_element_type=jnp.float32)


def attention_kernel(group, pack, aliased, *refs):
    q_ref, g_ref, k_ref, v_ref, bias_ref = refs[:5]
    out_ref, gq_ref, terms_ref, dk_ref, dv_ref = refs[7:] if aliased else refs[5:]
    scale = HEAD ** (-0.5)
    rows = q_ref.shape[1]
    k, v = k_ref[...], v_ref[...]
    k_t, v_t = k.T, v.T
    for first in range(0, group, pack):
        cols = [slice((first + j) * HEAD, (first + j + 1) * HEAD) for j in range(pack)]
        q = jnp.concatenate([q_ref[0, :, c] for c in cols], axis=0)
        g = jnp.concatenate([g_ref[0, :, c] for c in cols], axis=0)
        scores = times(k, q, ((1,), (1,))) * scale + bias_ref[...]
        expd = jnp.exp(scores - jnp.max(scores, axis=0, keepdims=True))
        probs = (expd * (1.0 / jnp.sum(expd, axis=0, keepdims=True))).astype(jnp.bfloat16)
        attended = times(v_t, probs, ((1,), (0,))).T
        dprob = times(v, g, ((1,), (1,)))
        wide = probs.astype(jnp.float32)
        delta = jnp.sum(wide * dprob, axis=0, keepdims=True)
        dscore = (wide * (dprob - delta)).astype(jnp.bfloat16)
        dquery = times(k_t, dscore, ((1,), (0,))).T
        out = (q.astype(jnp.float32) + attended).astype(jnp.bfloat16)
        gq = (g.astype(jnp.float32) + dquery * scale).astype(jnp.bfloat16)
        for j, c in enumerate(cols):
            out_ref[0, :, c] = out[j * rows : (j + 1) * rows]
            gq_ref[0, :, c] = gq[j * rows : (j + 1) * rows]
        dk = times(dscore, q, ((1,), (0,)))
        dv = times(probs, g, ((1,), (0,)))
        if first == 0:
            dk_ref[...] = dk
            dv_ref[...] = dv
        else:
            dk_ref[...] += dk
            dv_ref[...] += dv
    terms_ref[:, :HEAD] = (dk_ref[...] * scale).astype(jnp.bfloat16)
    terms_ref[:, HEAD:] = dv_ref[...].astype(jnp.bfloat16)


def attention(query, cotan, key_all, value_all, bias, head0, heads, whole_shape, partial):
    tok = query.shape[1]
    count = key_all.shape[0]
    width = query.shape[2] // heads
    group = width // HEAD
    pack = bias.shape[1] // tok
    aliased = partial is not None
    any_spec = pl.BlockSpec(memory_space=pl.ANY)
    chunk = pl.BlockSpec((1, tok, width), lambda h: (0, 0, h))
    kv = pl.BlockSpec((count, HEAD), lambda h: (0, head0 + h))
    result = pl.BlockSpec((1, tok, width), lambda h: (0, 0, head0 + h))
    pairs = group * heads * tok * count
    return pl.pallas_call(
        functools.partial(attention_kernel, group, pack, aliased),
        grid=(heads,),
        out_shape=(
            jax.ShapeDtypeStruct(whole_shape, jnp.bfloat16),
            jax.ShapeDtypeStruct(whole_shape, jnp.bfloat16),
            jax.ShapeDtypeStruct((count, heads * 2 * HEAD), jnp.bfloat16),
        ),
        in_specs=[chunk, chunk, kv, kv, pl.BlockSpec(bias.shape, lambda h: (0, 0))]
        + [any_spec, any_spec] * aliased,
        out_specs=(result, result, pl.BlockSpec((count, 2 * HEAD), lambda h: (0, h))),
        scratch_shapes=[pltpu.VMEM((count, HEAD), jnp.float32)] * 2,
        input_output_aliases={5: 0, 6: 1} if aliased else {},
        compiler_params=pltpu.CompilerParams(vmem_limit_bytes=48 * 1024 * 1024),
        cost_estimate=pl.CostEstimate(
            flops=12 * HEAD * pairs,
            bytes_accessed=8 * tok * width * heads + 8 * count * heads * HEAD,
            transcendentals=pairs,
        ),
    )(query, cotan, key_all, value_all, bias, *(partial if aliased else ()))


def summed_over(terms, axis, tok):
    devices = lax.axis_size(axis)
    me = lax.axis_index(axis)
    total = lax.dynamic_slice_in_dim(terms, me * tok, tok).astype(jnp.float32)
    for step in range(1, devices):
        there = lax.rem(me + step, devices)
        block = lax.dynamic_slice_in_dim(terms, there * tok, tok)
        total = total + passed_along(block, axis, step).astype(jnp.float32)
    return total


def on_device(acts, keys, values, grads, docs, order):
    tok = acts.shape[1]
    kv_count = keys.shape[2] // HEAD
    width = acts.shape[2] // kv_count
    group = width // HEAD
    pack = 2 if group % 2 == 0 else 1
    chunks = 2 if kv_count % 2 == 0 else 1
    heads = kv_count // chunks
    moved = []
    for c in range(chunks):
        cols = slice(c * heads * width, (c + 1) * heads * width)
        moved.append(
            (
                passed_along(acts[:, :, cols], "section", 1),
                passed_along(grads[:, :, cols], "section", -1),
            )
        )
    key_all = lax.all_gather(keys[0], "cp", axis=0, tiled=True)
    value_all = lax.all_gather(values[0], "cp", axis=0, tiled=True)

    positions = order[0]
    starts = jnp.sum(docs[0][None, :] < jnp.arange(1, DOCS)[:, None], axis=1)
    first = lax.axis_index("cp") * tok
    mine = lax.dynamic_slice_in_dim(positions, first, tok)
    low = jnp.max(jnp.where(starts[:, None] <= mine[None, :], starts[:, None], 0), axis=0)
    allowed = (positions[:, None] <= mine[None, :]) & (positions[:, None] >= low[None, :])
    bias = jnp.tile(jnp.where(allowed, 0.0, -1e30).astype(jnp.float32), (1, pack))

    partial, parts = None, []
    for c, (query, cotan) in enumerate(moved):
        out, gq, terms = attention(
            query, cotan, key_all, value_all, bias, c * heads, heads, acts.shape, partial
        )
        partial = (out, gq)
        parts.append(summed_over(terms, "cp", tok).astype(jnp.bfloat16))
    total = jnp.concatenate(parts, axis=1).reshape(tok, kv_count, 2, HEAD)
    grad_keys = total[:, :, 0].reshape(tok, kv_count * HEAD)
    grad_values = total[:, :, 1].reshape(tok, kv_count * HEAD)
    return (partial[0], partial[1], grad_keys[None], grad_values[None])


def solution(mesh):
    placed = (
        P("section", "cp", "tp"),
        P("section", "cp", "tp"),
        P("section", "cp", "tp"),
        P("section", "cp", "tp"),
        P("section", None),
        P("section", None),
    )
    return jax.shard_map(
        on_device,
        mesh=mesh,
        in_specs=placed,
        out_specs=(
            P("section", "cp", "tp"),
            P("section", "cp", "tp"),
            P("section", "cp", "tp"),
            P("section", "cp", "tp"),
        ),
        check_vma=False,
    )
```

```python
import functools

import jax
import jax.numpy as jnp
from jax import lax
from jax.experimental import pallas as pl
from jax.experimental.pallas import tpu as pltpu
from jax.sharding import PartitionSpec as P

HEAD = 128
DOCS = 8


def passed_along(block, axis, distance):
    devices = range(lax.axis_size(axis))
    route = [((i - distance) % len(devices), i) for i in devices]
    return lax.ppermute(block, axis, route)


def times(a, b, dims):
    return lax.dot_general(a, b, (dims, ((), ())), preferred_element_type=jnp.float32)


def attention_kernel(group, pack, blocks, aliased, *refs):
    q_ref, g_ref, bias_ref = refs[:3]
    k_refs, v_refs = refs[3 : 3 + blocks], refs[3 + blocks : 3 + 2 * blocks]
    out_ref, gq_ref, terms_ref, dk_ref, dv_ref = refs[-5:]
    scale = HEAD ** (-0.5)
    rows = q_ref.shape[1]
    k = jnp.concatenate([ref[...] for ref in k_refs], axis=0)
    v = jnp.concatenate([ref[...] for ref in v_refs], axis=0)
    bias = jnp.concatenate([bias_ref[...]] * pack, axis=1)
    k_t, v_t = k.T, v.T
    for first in range(0, group, pack):
        cols = [slice((first + j) * HEAD, (first + j + 1) * HEAD) for j in range(pack)]
        q = jnp.concatenate([q_ref[0, :, c] for c in cols], axis=0)
        g = jnp.concatenate([g_ref[0, :, c] for c in cols], axis=0)
        scores = times(k, q, ((1,), (1,))) * scale + bias
        expd = jnp.exp(scores - jnp.max(scores, axis=0, keepdims=True))
        probs = (expd * (1.0 / jnp.sum(expd, axis=0, keepdims=True))).astype(jnp.bfloat16)
        attended = times(v_t, probs, ((1,), (0,))).T
        dprob = times(v, g, ((1,), (1,)))
        wide = probs.astype(jnp.float32)
        delta = jnp.sum(wide * dprob, axis=0, keepdims=True)
        dscore = (wide * (dprob - delta)).astype(jnp.bfloat16)
        dquery = times(k_t, dscore, ((1,), (0,))).T
        out = (q.astype(jnp.float32) + attended).astype(jnp.bfloat16)
        gq = (g.astype(jnp.float32) + dquery * scale).astype(jnp.bfloat16)
        for j, c in enumerate(cols):
            out_ref[0, :, c] = out[j * rows : (j + 1) * rows]
            gq_ref[0, :, c] = gq[j * rows : (j + 1) * rows]
        dk = times(dscore, q, ((1,), (0,)))
        dv = times(probs, g, ((1,), (0,)))
        if first == 0:
            dk_ref[...] = dk
            dv_ref[...] = dv
        else:
            dk_ref[...] += dk
            dv_ref[...] += dv
    terms_ref[:, :HEAD] = (dk_ref[...] * scale).astype(jnp.bfloat16)
    terms_ref[:, HEAD:] = dv_ref[...].astype(jnp.bfloat16)


def attention(query, cotan, held, bias, head0, heads, whole_shape, partial):
    tok = query.shape[1]
    blocks = len(held)
    count = blocks * tok
    kv_count = held[0].shape[1] // (2 * HEAD)
    width = query.shape[2] // heads
    group = width // HEAD
    pack = 2 if group % 2 == 0 else 1
    aliased = partial is not None
    any_spec = pl.BlockSpec(memory_space=pl.ANY)
    chunk = pl.BlockSpec((1, tok, width), lambda h: (0, 0, h))
    key = pl.BlockSpec((tok, HEAD), lambda h: (0, head0 + h))
    value = pl.BlockSpec((tok, HEAD), lambda h: (0, kv_count + head0 + h))
    result = pl.BlockSpec((1, tok, width), lambda h: (0, 0, head0 + h))
    pairs = group * heads * tok * count
    return pl.pallas_call(
        functools.partial(attention_kernel, group, pack, blocks, aliased),
        grid=(heads,),
        out_shape=(
            jax.ShapeDtypeStruct(whole_shape, jnp.bfloat16),
            jax.ShapeDtypeStruct(whole_shape, jnp.bfloat16),
            jax.ShapeDtypeStruct((count, heads * 2 * HEAD), jnp.bfloat16),
        ),
        in_specs=[chunk, chunk, pl.BlockSpec(bias.shape, lambda h: (0, 0))]
        + [key] * blocks
        + [value] * blocks
        + [any_spec, any_spec] * aliased,
        out_specs=(result, result, pl.BlockSpec((count, 2 * HEAD), lambda h: (0, h))),
        scratch_shapes=[pltpu.VMEM((count, HEAD), jnp.float32)] * 2,
        input_output_aliases={3 + 2 * blocks: 0, 4 + 2 * blocks: 1} if aliased else {},
        compiler_params=pltpu.CompilerParams(vmem_limit_bytes=48 * 1024 * 1024),
        cost_estimate=pl.CostEstimate(
            flops=12 * HEAD * pairs,
            bytes_accessed=8 * tok * width * heads + 8 * count * heads * HEAD,
            transcendentals=pairs,
        ),
    )(query, cotan, bias, *held, *held, *(partial if aliased else ()))


def summed_over(terms, axis, tok):
    total = terms[:tok].astype(jnp.float32)
    for back in range(1, lax.axis_size(axis)):
        block = terms[back * tok : (back + 1) * tok]
        total = total + passed_along(block, axis, -back).astype(jnp.float32)
    return total


def on_device(acts, keys, values, grads, docs, order):
    tok = acts.shape[1]
    kv_count = keys.shape[2] // HEAD
    width = acts.shape[2] // kv_count
    chunks, heads = kv_count, 1
    own = jnp.concatenate([keys[0], values[0]], axis=1)
    held = [own] + [
        passed_along(own, "cp", back) for back in range(1, lax.axis_size("cp"))
    ]
    moved = []
    for c in range(chunks):
        cols = slice(c * heads * width, (c + 1) * heads * width)
        moved.append(
            (
                passed_along(acts[:, :, cols], "section", 1),
                passed_along(grads[:, :, cols], "section", -1),
            )
        )
    positions = order[0]
    starts = jnp.sum(docs[0][None, :] < jnp.arange(1, DOCS)[:, None], axis=1)
    first = lax.axis_index("cp") * tok
    mine = lax.dynamic_slice_in_dim(positions, first, tok)
    low = jnp.max(jnp.where(starts[:, None] <= mine[None, :], starts[:, None], 0), axis=0)
    blocks = lax.axis_size("cp")
    met = [
        lax.dynamic_slice_in_dim(
            positions, lax.rem(lax.axis_index("cp") + blocks - back, blocks) * tok, tok
        )
        for back in range(blocks)
    ]
    met = jnp.concatenate(met)
    allowed = (met[:, None] <= mine[None, :]) & (met[:, None] >= low[None, :])
    bias = jnp.where(allowed, 0.0, -1e30).astype(jnp.float32)

    partial, parts = None, []
    for c, (query, cotan) in enumerate(moved):
        out, gq, terms = attention(
            query, cotan, held, bias, c * heads, heads, acts.shape, partial
        )
        partial = (out, gq)
        parts.append(summed_over(terms, "cp", tok).astype(jnp.bfloat16))
    total = jnp.concatenate(parts, axis=1).reshape(tok, kv_count, 2, HEAD)
    grad_keys = total[:, :, 0].reshape(tok, kv_count * HEAD)
    grad_values = total[:, :, 1].reshape(tok, kv_count * HEAD)
    return (partial[0], partial[1], grad_keys[None], grad_values[None])


def solution(mesh):
    placed = (
        P("section", "cp", "tp"),
        P("section", "cp", "tp"),
        P("section", "cp", "tp"),
        P("section", "cp", "tp"),
        P("section", None),
        P("section", None),
    )
    return jax.shard_map(
        on_device,
        mesh=mesh,
        in_specs=placed,
        out_specs=(
            P("section", "cp", "tp"),
            P("section", "cp", "tp"),
            P("section", "cp", "tp"),
            P("section", "cp", "tp"),
        ),
        check_vma=False,
    )
```
